256 devices in a mesh: groups: 4 (over y, x), tensor: 32 (over z), seq: 2 (over core).
Axes of the slice: x: 2, y: 2, z: 32, core: 2. Of those that a mesh axis runs over, the one named last changes fastest.
The devices are a block of a 4x8x32 slice.
Arguments:
- queries: bfloat16 [128, 64, 128], P('groups'), parts along dimension 0
- keys: bfloat16 [32768, 128, 128], P(('tensor', 'seq'), 'groups'), parts along dimension 1
- values: bfloat16 [32768, 128, 128], P(('tensor', 'seq'), 'groups'), parts along dimension 1, may hold values from -6 to 6
- lengths: int32 [128], P('groups'), parts along dimension 0, may hold values from 2 to 4096, as said below
- out_weight: bfloat16 [8192, 8192], P(('tensor', 'seq')), may hold values from -1.5 to 1.5
Outputs:
- mixed: bfloat16 [128, 8192], P('groups', ('tensor', 'seq')), parts along dimension 0
The draws below stay inside these ranges and needn't reach their ends.
There are 4 independent parts, one for each index of `groups`. The reference program is written for one: setup_inputs(seed, part) draws one part's arguments, and reference() takes and returns one part's arrays. A program takes and returns all parts, laid end to end along the dimension named above; an argument that names none is the same for every part. Nothing has to cross between parts.
Inputs may be any that keep to these rules, and one draw needn't show every extreme that they name: `lengths`: every length is at least 2, and in each part one sequence has exactly 4096 live slots.
All inputs are finite; a program needn't handle non-finite values.
Results may differ from the reference program's by a relative error of at most 0.005.
Values sent between devices are 32-bit elements; how exact they have to be, the bound alone decides.
No kernel may reach another device: no remote copies, remote signals or barrier semaphores. Data moves between devices by JAX's collectives and lax.ppermute only.
A program may use at most 64 MiB of HBM per device.

```python
import jax
import jax.numpy as jnp
from jax import lax

D = 8192
HQ = 64
KVH = 8
HD = 128
BATCH = 32
CACHE = 4096


def draw_queries(key, part):
    base = 1.5 * jax.random.normal(jax.random.fold_in(key, 11), (BATCH, HQ, HD), jnp.float32)
    return base.astype(jnp.bfloat16)


def draw_keys(key, part):
    base = jax.random.normal(jax.random.fold_in(key, 22), (KVH * CACHE, BATCH, HD), jnp.float32)
    return base.astype(jnp.bfloat16)


def draw_lengths(key, part):
    spread = jax.random.randint(jax.random.fold_in(key, 31), (BATCH,), 2, CACHE + 1)
    chosen = jax.random.randint(jax.random.fold_in(key, 32), (), 0, BATCH)
    return jnp.where(jnp.arange(BATCH) == chosen, CACHE, spread).astype(jnp.int32)


def raised(result, stream_key, source, target, parts, factor):
    owner, partner = [(jnp.arange(result.shape[axis_at]) // (result.shape[axis_at] // parts)).reshape([-1 if axis == axis_at else 1 for axis in range(result.ndim)]) for axis_at in (source, target)]
    chosen = jax.random.permutation(stream_key, parts)[partner]
    strong = (owner == chosen) | (owner == (partner + parts // 2) % parts)
    return jnp.where(strong, factor * result, result)


def block_scale(key, dims, cuts, least, high):
    loudness, own = 1.0, jax.random.fold_in(key, 6)
    for axis_at, shards_of in cuts:
        draws = jnp.exp(jax.random.uniform(jax.random.fold_in(own, axis_at), (shards_of,), jnp.float32, least / len(cuts), high / len(cuts)))
        loudness = loudness * jnp.repeat(draws, dims[axis_at] // shards_of).reshape([-1 if axis == axis_at else 1 for axis in range(len(dims))])
    return loudness


def scatter_about(own_key, shape, scale, most, pieces=(), kind=jnp.bfloat16):
    entries = scale * jax.random.normal(own_key, shape, jnp.float32)
    if pieces:
        entries = entries * block_scale(own_key, shape, pieces, -0.22, 0.18)
    return jnp.clip(entries, -most, most).astype(kind)


def heavy_noise(rng, shape, scale, most, cuts, heavy, held_as=jnp.bfloat16):
    result = scale * jax.random.normal(rng, shape, jnp.float32)
    if cuts:
        result = result * block_scale(rng, shape, cuts, -0.22, 0.18)
    return jnp.clip(raised(result, jax.random.fold_in(rng, 3), *heavy), -most, most).astype(held_as)


def setup_inputs(seed: int = 0, part: int = 0) -> dict:
    arg_keys = jax.random.split(jax.random.key(seed), 6)
    part_keys = jax.random.split(jax.random.fold_in(arg_keys[5], part), 6)
    queries = draw_queries(jax.random.fold_in(jax.random.fold_in(arg_keys[5], part), 71), part)
    keys = draw_keys(jax.random.fold_in(jax.random.fold_in(arg_keys[5], part), 71), part)
    values = scatter_about(part_keys[2], (KVH * CACHE, BATCH, HD), 1.0, 6.0, ((0, 64),))
    lengths = draw_lengths(jax.random.fold_in(jax.random.fold_in(arg_keys[5], part), 71), part)
    out_weight = heavy_noise(arg_keys[4], (HQ * HD, D), HD ** -0.5, 1.5, ((0, 64),), (0, 1, 64, 4.0))
    return {"queries": queries, "keys": keys, "values": values, "lengths": lengths, "out_weight": out_weight}


masked_fill = -1e+30

def reference(queries, keys, values, lengths, out_weight):
    per_group = HQ // KVH
    positions = jnp.arange(CACHE, dtype=jnp.int32)
    live = (positions[None, :] < lengths[:, None])[:, None, :]
    results = []
    for head in range(KVH):
        head_keys = keys[head * CACHE:(head + 1) * CACHE].astype(jnp.float32)
        head_values = values[head * CACHE:(head + 1) * CACHE].astype(jnp.float32)
        head_queries = queries[:, head * per_group:(head + 1) * per_group].astype(jnp.float32)
        scores = jnp.einsum('bgd,pbd->bgp', head_queries, head_keys, precision=lax.Precision.HIGHEST) / jnp.sqrt(jnp.float32(HD))
        scores = jnp.where(live, scores, masked_fill)
        highest = lax.optimization_barrier(jnp.max(scores, axis=2))
        weights = jnp.where(live, jnp.exp(scores - highest[..., None]), 0.0)
        totals = lax.optimization_barrier(jnp.sum(weights, axis=2))
        accum = jnp.einsum('bgp,pbd->bgd', weights, head_values, precision=lax.Precision.HIGHEST)
        results.append(accum / totals[..., None])
    attended = jnp.concatenate(results, axis=1).reshape(BATCH, HQ * HD).astype(jnp.bfloat16)
    return jnp.dot(attended, out_weight, preferred_element_type=jnp.float32).astype(jnp.bfloat16)
```

```python
import functools
import math

import jax
import jax.numpy as jnp
from jax import lax
from jax.experimental import pallas as pl
from jax.experimental.pallas import tpu as pltpu
from jax.sharding import PartitionSpec as P

KVH = 8
CACHE = 4096
masked_fill = -1e30
ROWS = 8
LANES = 128


def attend_kernel(
    replicas, lengths_ref, q_hbm, k_ref, v_ref, keep_ref, send_ref, q_raw, q_all, s_ref, stats_ref, sem
):
    step = pl.program_id(0)
    tensor_index = lax.axis_index("tensor")
    seq_index = lax.axis_index("seq")
    n_seq = lax.axis_size("seq")
    span = k_ref.shape[0]
    batch, group, head_size = q_raw.shape
    start = (tensor_index * n_seq + seq_index) * span
    kv_head = start // CACHE
    first_slot = start % CACHE
    own = tensor_index % replicas

    @pl.when(step == 0)
    def _():
        heads = pl.ds(pl.multiple_of(kv_head * group, group), group)
        copy = pltpu.make_async_copy(q_hbm.at[:, heads, :], q_raw, sem)
        copy.start()
        copy.wait()
        q_all[...] = q_raw[...].astype(jnp.float32).reshape(batch * group, head_size)
        stats_ref[...] = jnp.zeros_like(stats_ref)

    base = pl.multiple_of(step * ROWS * group, ROWS * group)
    pieces = []
    for place in range(group):
        which, rank = place // replicas, place % replicas
        head = 2 * (own ^ rank) + (seq_index ^ which)
        pieces.append(q_all[pl.ds(base + head, ROWS, stride=group), :])
    queries = jnp.concatenate(pieces, axis=0).astype(jnp.bfloat16)

    row = lax.broadcasted_iota(jnp.int32, (ROWS, LANES), 0)
    lane = lax.broadcasted_iota(jnp.int32, (ROWS, LANES), 1)
    left = jnp.zeros((ROWS, LANES), jnp.int32)
    for r in range(ROWS):
        left = jnp.where(row == r, lengths_ref[step * ROWS + r] - first_slot, left)
    place_of = jnp.where(lane % ROWS == row, lane // ROWS, CACHE)
    slots = LANES // ROWS
    blocks = span // slots
    per_dot = 4
    scale = math.log2(math.e) / math.sqrt(head_size)
    width = per_dot * LANES

    highest = jnp.full((group * ROWS, LANES), masked_fill, jnp.float32)
    for c in range(blocks // per_dot):
        keys = k_ref[c * per_dot * slots : (c + 1) * per_dot * slots].reshape(width, head_size)
        scores = lax.dot_general(
            queries, keys, (((1,), (1,)), ((), ())), preferred_element_type=jnp.float32
        )
        for j in range(per_dot):
            live = place_of < left - (c * per_dot + j) * slots
            live = jnp.concatenate([live] * group, axis=0)
            part = jnp.where(live, scores[:, j * LANES : (j + 1) * LANES] * scale, masked_fill)
            s_ref[c * per_dot + j] = part
            highest = jnp.maximum(highest, part)
    top = jnp.max(highest, axis=1, keepdims=True)
    total = jnp.zeros((group * ROWS, LANES), jnp.float32)
    accum = jnp.zeros((group * ROWS, head_size), jnp.float32)
    for c in range(blocks // per_dot):
        parts = []
        for j in range(per_dot):
            live = place_of < left - (c * per_dot + j) * slots
            live = jnp.concatenate([live] * group, axis=0)
            weight = jnp.where(live, jnp.exp2(s_ref[c * per_dot + j] - top), 0.0)
            total = total + weight
            parts.append(weight.astype(jnp.bfloat16))
        values = v_ref[c * per_dot * slots : (c + 1) * per_dot * slots].reshape(width, head_size)
        accum = accum + jnp.dot(
            jnp.concatenate(parts, axis=1), values, preferred_element_type=jnp.float32
        )
    total = jnp.sum(total, axis=1, keepdims=True)
    for place in range(group):
        which, rank = place // replicas, place % replicas
        ref = (keep_ref, send_ref)[which]
        rows = slice(place * ROWS, (place + 1) * ROWS)
        ref[rank, pl.ds(pl.multiple_of(step * ROWS, ROWS), ROWS), :] = accum[rows]
        spread = jnp.where(lane == row + step * ROWS, top[rows], 0.0)
        spread = jnp.where(lane == row + step * ROWS + batch, total[rows], spread)
        stats_ref[place] += spread

    @pl.when(step == pl.num_programs(0) - 1)
    def _():
        for place in range(group):
            which, rank = place // replicas, place % replicas
            ref = (keep_ref, send_ref)[which]
            line = jnp.sum(stats_ref[place], axis=0, keepdims=True)
            ref[rank, batch:, :] = jnp.broadcast_to(line, (ROWS, LANES))


def column(line, batch):
    row = lax.broadcasted_iota(jnp.int32, (batch, LANES), 0)
    lane = lax.broadcasted_iota(jnp.int32, (batch, LANES), 1)
    return jnp.sum(jnp.where(lane == row, line, 0.0), axis=1, keepdims=True)


def merge_kernel(keep_ref, got_ref, *out_refs):
    batch = keep_ref.shape[1] - ROWS
    lane = lax.broadcasted_iota(jnp.int32, (1, LANES), 1)
    for rank, out_ref in enumerate(out_refs):
        first = keep_ref[rank, batch : batch + 1, :]
        second = got_ref[rank, batch : batch + 1, :]
        top = jnp.maximum(first, second)
        scale_a = jnp.where(lane < batch, jnp.exp2(first - top), 0.0)
        scale_b = jnp.where(lane < batch, jnp.exp2(second - top), 0.0)
        total = first * pltpu.roll(scale_a, batch, 1) + second * pltpu.roll(scale_b, batch, 1)
        out_ref[:batch, :] = keep_ref[rank, :batch, :] * column(scale_a, batch) + got_ref[
            rank, :batch, :
        ] * column(scale_b, batch)
        out_ref[batch:, :] = jnp.broadcast_to(jnp.where(lane < batch, top, total), (ROWS, LANES))


def project_kernel(reach, w_ref, *refs):
    *parts, odd_ref, rest_ref, odd_send_ref, rest_send_ref = refs
    tensor_index = lax.axis_index("tensor")
    seq_index = lax.axis_index("seq")
    n_tensor = lax.axis_size("tensor")
    batch = parts[0].shape[0] - ROWS
    lane = lax.broadcasted_iota(jnp.int32, (1, LANES), 1)
    lines = [ref[batch : batch + 1, :] for ref in parts]
    top = functools.reduce(jnp.maximum, lines)
    scales = [jnp.where(lane < batch, jnp.exp2(line - top), 0.0) for line in lines]
    total = sum(line * pltpu.roll(scale, batch, 1) for line, scale in zip(lines, scales))
    total = pltpu.roll(total, LANES - batch, 1)
    accum = sum(ref[:batch, :] * column(scale, batch) for ref, scale in zip(parts, scales))
    mean = accum / column(jnp.where(lane < batch, total, 0.0), batch)
    attended = mean.astype(jnp.bfloat16)
    width = odd_ref.shape[2]
    odd, rest = orders(reach)
    for own_side in (0, 1):
        up = (seq_index ^ 1 ^ own_side) == 1
        for order, ref in (
            (odd, (odd_send_ref, odd_ref)[own_side]),
            (rest, (rest_send_ref, rest_ref)[own_side]),
        ):
            for place, distance in enumerate(order):
                hop = jnp.where(up, distance, n_tensor - distance)
                chip = lax.rem(tensor_index + hop, n_tensor)
                down_is_live = 1 <= distance <= n_tensor - reach
                columns = pl.ds(pl.multiple_of(chip * width, width), width)
                block = jnp.dot(attended, w_ref[:, columns], preferred_element_type=jnp.float32)
                if not down_is_live:
                    block = jnp.where(up, block, 0.0)
                ref[place] = block


def orders(reach):
    odd = [*range(3, reach, 4), *range(1, reach, 4)]
    rest = [*range(2, reach, 4), *range(0, reach, 4)]
    return odd, rest


def other_core(block):
    return lax.ppermute(block, "seq", [(0, 1), (1, 0)])


def across(block, mask):
    count = lax.axis_size("tensor")
    return lax.ppermute(block, "tensor", [(i, i ^ mask) for i in range(count)])


def onward(block, hops):
    count = lax.axis_size("tensor")
    route = []
    for chip in range(count):
        route.append((2 * chip + 1, 2 * ((chip + hops) % count) + 1))
        route.append((2 * chip, 2 * ((chip - hops) % count)))
    return lax.ppermute(block, ("tensor", "seq"), route)


def body(queries, keys, values, lengths, out_weight):
    n_tensor = lax.axis_size("tensor")
    n_seq = lax.axis_size("seq")
    replicas = n_tensor // KVH
    seq_index = lax.axis_index("seq")
    span, batch, head_size = keys.shape
    group = queries.shape[1] // KVH
    any_space = pl.BlockSpec(memory_space=pl.ANY)
    vmem = pl.BlockSpec(memory_space=pltpu.VMEM)
    state = jax.ShapeDtypeStruct((replicas, batch + ROWS, head_size), jnp.float32)
    piece = jax.ShapeDtypeStruct((batch + ROWS, head_size), jnp.float32)
    whole = pl.BlockSpec(state.shape, lambda i: (0, 0, 0))
    cache = pl.BlockSpec((span, ROWS, head_size), lambda i: (0, i, 0))
    keep, send = pl.pallas_call(
        functools.partial(attend_kernel, replicas),
        grid=(batch // ROWS,),
        out_shape=[state, state],
        in_specs=[pl.BlockSpec(memory_space=pltpu.SMEM), any_space, cache, cache],
        out_specs=[whole, whole],
        scratch_shapes=[
            pltpu.VMEM((batch, group, head_size), jnp.bfloat16),
            pltpu.VMEM((batch * group, head_size), jnp.float32),
            pltpu.VMEM((span * ROWS // LANES, group * ROWS, LANES), jnp.float32),
            pltpu.VMEM((group, ROWS, LANES), jnp.float32),
            pltpu.SemaphoreType.DMA,
        ],
        compiler_params=pltpu.CompilerParams(vmem_limit_bytes=24 << 20),
        name="attend",
    )(lengths, queries, keys, values)
    got = other_core(send)
    merged = pl.pallas_call(
        merge_kernel,
        out_shape=[piece] * replicas,
        in_specs=[vmem, vmem],
        out_specs=[vmem] * replicas,
        name="merge",
    )(keep, got)
    parts = [merged[0]] + [across(merged[mask], mask) for mask in range(1, replicas)]

    width = out_weight.shape[1] // n_tensor
    reach = 20
    odd, rest = orders(reach)
    chunks = lambda order: jax.ShapeDtypeStruct((len(order), batch, width), jnp.float32)
    odd_own, rest_own, odd_send, rest_send = pl.pallas_call(
        functools.partial(project_kernel, reach),
        out_shape=[chunks(odd), chunks(rest), chunks(odd), chunks(rest)],
        in_specs=[vmem] * (1 + replicas),
        out_specs=[vmem] * 4,
        compiler_params=pltpu.CompilerParams(vmem_limit_bytes=16 << 20),
        name="project",
    )(out_weight, *parts)
    odd_sum = odd_own + other_core(odd_send)
    rest_got = other_core(rest_send)
    twos = len(range(2, reach, 4))
    first = onward(odd_sum, 1)
    even = rest_own[:twos] + rest_got[:twos] + first[:twos]
    fours = rest_own[twos:] + rest_got[twos:] + first[twos:]
    second = onward(even, 2)
    last = fours.shape[0] - 1
    carry = fours[last] + second[last]
    for place in reversed(range(last)):
        carry = onward(carry, 4) + (fours[place] + second[place])
    half = width // n_seq
    mine = jnp.where(seq_index == 1, carry[:, half:], carry[:, :half])
    theirs = jnp.where(seq_index == 1, carry[:, :half], carry[:, half:])
    return (mine + other_core(theirs)).astype(jnp.bfloat16)


def solution(mesh):
    return jax.shard_map(
        body,
        mesh=mesh,
        in_specs=(
            P("groups", None, None),
            P(("tensor", "seq"), "groups", None),
            P(("tensor", "seq"), "groups", None),
            P("groups"),
            P(("tensor", "seq"), None),
        ),
        out_specs=P("groups", ("tensor", "seq")),
        check_vma=False,
    )
```

```python
import functools
import math

import jax
import jax.numpy as jnp
from jax import lax
from jax.experimental import pallas as pl
from jax.experimental.pallas import tpu as pltpu
from jax.sharding import PartitionSpec as P

KVH = 8
CACHE = 4096
masked_fill = -1e30
ROWS = 8
LANES = 128


def attend_kernel(
    replicas, lengths_ref, q_hbm, k_ref, v_ref, keep_ref, send_ref, q_raw, q_all, s_ref, stats_ref, sem
):
    step = pl.program_id(0)
    tensor_index = lax.axis_index("tensor")
    seq_index = lax.axis_index("seq")
    n_seq = lax.axis_size("seq")
    span = k_ref.shape[0]
    batch, group, head_size = q_raw.shape
    start = (tensor_index * n_seq + seq_index) * span
    kv_head = start // CACHE
    first_slot = start % CACHE
    own = tensor_index % replicas

    @pl.when(step == 0)
    def _():
        heads = pl.ds(pl.multiple_of(kv_head * group, group), group)
        copy = pltpu.make_async_copy(q_hbm.at[:, heads, :], q_raw, sem)
        copy.start()
        copy.wait()
        q_all[...] = q_raw[...].astype(jnp.float32).reshape(batch * group, head_size)
        stats_ref[...] = jnp.zeros_like(stats_ref)

    base = pl.multiple_of(step * ROWS * group, ROWS * group)
    pieces = []
    for place in range(group):
        which, rank = place // replicas, place % replicas
        head = 2 * (own ^ rank) + (seq_index ^ which)
        pieces.append(q_all[pl.ds(base + head, ROWS, stride=group), :])
    queries = jnp.concatenate(pieces, axis=0).astype(jnp.bfloat16)

    row = lax.broadcasted_iota(jnp.int32, (ROWS, LANES), 0)
    lane = lax.broadcasted_iota(jnp.int32, (ROWS, LANES), 1)
    left = jnp.zeros((ROWS, LANES), jnp.int32)
    for r in range(ROWS):
        left = jnp.where(row == r, lengths_ref[step * ROWS + r] - first_slot, left)
    place_of = jnp.where(lane % ROWS == row, lane // ROWS, CACHE)
    slots = LANES // ROWS
    blocks = span // slots
    per_dot = 4
    scale = math.log2(math.e) / math.sqrt(head_size)
    width = per_dot * LANES

    highest = jnp.full((group * ROWS, LANES), masked_fill, jnp.float32)
    for c in range(blocks // per_dot):
        keys = k_ref[c * per_dot * slots : (c + 1) * per_dot * slots].reshape(width, head_size)
        scores = lax.dot_general(
            queries, keys, (((1,), (1,)), ((), ())), preferred_element_type=jnp.float32
        )
        for j in range(per_dot):
            live = place_of < left - (c * per_dot + j) * slots
            live = jnp.concatenate([live] * group, axis=0)
            part = jnp.where(live, scores[:, j * LANES : (j + 1) * LANES] * scale, masked_fill)
            s_ref[c * per_dot + j] = part
            highest = jnp.maximum(highest, part)
    top = jnp.max(highest, axis=1, keepdims=True)
    total = jnp.zeros((group * ROWS, LANES), jnp.float32)
    accum = jnp.zeros((group * ROWS, head_size), jnp.float32)
    for c in range(blocks // per_dot):
        parts = []
        for j in range(per_dot):
            live = place_of < left - (c * per_dot + j) * slots
            live = jnp.concatenate([live] * group, axis=0)
            weight = jnp.where(live, jnp.exp2(s_ref[c * per_dot + j] - top), 0.0)
            total = total + weight
            parts.append(weight.astype(jnp.bfloat16))
        values = v_ref[c * per_dot * slots : (c + 1) * per_dot * slots].reshape(width, head_size)
        accum = accum + jnp.dot(
            jnp.concatenate(parts, axis=1), values, preferred_element_type=jnp.float32
        )
    total = jnp.sum(total, axis=1, keepdims=True)
    for place in range(group):
        which, rank = place // replicas, place % replicas
        ref = (keep_ref, send_ref)[which]
        rows = slice(place * ROWS, (place + 1) * ROWS)
        ref[rank, pl.ds(pl.multiple_of(step * ROWS, ROWS), ROWS), :] = accum[rows]
        spread = jnp.where(lane == row + step * ROWS, top[rows], 0.0)
        spread = jnp.where(lane == row + step * ROWS + batch, total[rows], spread)
        stats_ref[place] += spread

    @pl.when(step == pl.num_programs(0) - 1)
    def _():
        for place in range(group):
            which, rank = place // replicas, place % replicas
            ref = (keep_ref, send_ref)[which]
            line = jnp.sum(stats_ref[place], axis=0, keepdims=True)
            ref[rank, batch:, :] = jnp.broadcast_to(line, (ROWS, LANES))


def column(line, batch):
    row = lax.broadcasted_iota(jnp.int32, (batch, LANES), 0)
    lane = lax.broadcasted_iota(jnp.int32, (batch, LANES), 1)
    return jnp.sum(jnp.where(lane == row, line, 0.0), axis=1, keepdims=True)


def merge_kernel(keep_ref, got_ref, *out_refs):
    batch = keep_ref.shape[1] - ROWS
    lane = lax.broadcasted_iota(jnp.int32, (1, LANES), 1)
    for rank, out_ref in enumerate(out_refs):
        first = keep_ref[rank, batch : batch + 1, :]
        second = got_ref[rank, batch : batch + 1, :]
        top = jnp.maximum(first, second)
        scale_a = jnp.where(lane < batch, jnp.exp2(first - top), 0.0)
        scale_b = jnp.where(lane < batch, jnp.exp2(second - top), 0.0)
        total = first * pltpu.roll(scale_a, batch, 1) + second * pltpu.roll(scale_b, batch, 1)
        out_ref[:batch, :] = keep_ref[rank, :batch, :] * column(scale_a, batch) + got_ref[
            rank, :batch, :
        ] * column(scale_b, batch)
        out_ref[batch:, :] = jnp.broadcast_to(jnp.where(lane < batch, top, total), (ROWS, LANES))


def project_kernel(reach, w_ref, *refs):
    *parts, odd_ref, rest_ref, odd_send_ref, rest_send_ref = refs
    tensor_index = lax.axis_index("tensor")
    seq_index = lax.axis_index("seq")
    n_tensor = lax.axis_size("tensor")
    batch = parts[0].shape[0] - ROWS
    lane = lax.broadcasted_iota(jnp.int32, (1, LANES), 1)
    lines = [ref[batch : batch + 1, :] for ref in parts]
    top = functools.reduce(jnp.maximum, lines)
    scales = [jnp.where(lane < batch, jnp.exp2(line - top), 0.0) for line in lines]
    total = sum(line * pltpu.roll(scale, batch, 1) for line, scale in zip(lines, scales))
    total = pltpu.roll(total, LANES - batch, 1)
    accum = sum(ref[:batch, :] * column(scale, batch) for ref, scale in zip(parts, scales))
    mean = accum / column(jnp.where(lane < batch, total, 0.0), batch)
    attended = mean.astype(jnp.bfloat16)
    width = odd_ref.shape[2]
    odd, rest = orders(reach)
    for own_side in (0, 1):
        up = (seq_index ^ 1 ^ own_side) == 1
        for order, ref in (
            (odd, (odd_send_ref, odd_ref)[own_side]),
            (rest, (rest_send_ref, rest_ref)[own_side]),
        ):
            for place, distance in enumerate(order):
                hop = jnp.where(up, distance, n_tensor - distance)
                chip = lax.rem(tensor_index + hop, n_tensor)
                down_is_live = 1 <= distance <= n_tensor - reach
                columns = pl.ds(pl.multiple_of(chip * width, width), width)
                block = jnp.dot(attended, w_ref[:, columns], preferred_element_type=jnp.float32)
                if not down_is_live:
                    block = jnp.where(up, block, 0.0)
                ref[place] = block


def orders(reach):
    odd = [*range(3, reach, 4), *range(1, reach, 4)]
    rest = [*range(2, reach, 4), *range(0, reach, 4)]
    return odd, rest


def other_core(block):
    return lax.ppermute(block, "seq", [(0, 1), (1, 0)])


def across(block, mask):
    count = lax.axis_size("tensor")
    return lax.ppermute(block, "tensor", [(i, i ^ mask) for i in range(count)])


def onward(block, hops):
    count = lax.axis_size("tensor")
    route = []
    for chip in range(count):
        route.append((2 * chip + 1, 2 * ((chip + hops) % count) + 1))
        route.append((2 * chip, 2 * ((chip - hops) % count)))
    return lax.ppermute(block, ("tensor", "seq"), route)


def body(queries, keys, values, lengths, out_weight):
    n_tensor = lax.axis_size("tensor")
    n_seq = lax.axis_size("seq")
    replicas = n_tensor // KVH
    seq_index = lax.axis_index("seq")
    span, batch, head_size = keys.shape
    group = queries.shape[1] // KVH
    any_space = pl.BlockSpec(memory_space=pl.ANY)
    vmem = pl.BlockSpec(memory_space=pltpu.VMEM)
    state = jax.ShapeDtypeStruct((replicas, batch + ROWS, head_size), jnp.float32)
    piece = jax.ShapeDtypeStruct((batch + ROWS, head_size), jnp.float32)
    whole = pl.BlockSpec(state.shape, lambda i: (0, 0, 0))
    cache = pl.BlockSpec((span, ROWS, head_size), lambda i: (0, i, 0))
    keep, send = pl.pallas_call(
        functools.partial(attend_kernel, replicas),
        grid=(batch // ROWS,),
        out_shape=[state, state],
        in_specs=[pl.BlockSpec(memory_space=pltpu.SMEM), any_space, cache, cache],
        out_specs=[whole, whole],
        scratch_shapes=[
            pltpu.VMEM((batch, group, head_size), jnp.bfloat16),
            pltpu.VMEM((batch * group, head_size), jnp.float32),
            pltpu.VMEM((span * ROWS // LANES, group * ROWS, LANES), jnp.float32),
            pltpu.VMEM((group, ROWS, LANES), jnp.float32),
            pltpu.SemaphoreType.DMA,
        ],
        compiler_params=pltpu.CompilerParams(vmem_limit_bytes=60 << 20),
        name="attend",
    )(lengths, queries, keys, values)
    got = other_core(send)
    merged = pl.pallas_call(
        merge_kernel,
        out_shape=[piece] * replicas,
        in_specs=[vmem, vmem],
        out_specs=[vmem] * replicas,
        compiler_params=pltpu.CompilerParams(vmem_limit_bytes=4 << 20),
        name="merge",
    )(keep, got)
    parts = [merged[0]] + [across(merged[mask], mask) for mask in range(1, replicas)]

    width = out_weight.shape[1] // n_tensor
    reach = 20
    odd, rest = orders(reach)
    chunks = lambda order: jax.ShapeDtypeStruct((len(order), batch, width), jnp.float32)
    odd_own, rest_own, odd_send, rest_send = pl.pallas_call(
        functools.partial(project_kernel, reach),
        out_shape=[chunks(odd), chunks(rest), chunks(odd), chunks(rest)],
        in_specs=[vmem] * (1 + replicas),
        out_specs=[vmem] * 4,
        compiler_params=pltpu.CompilerParams(vmem_limit_bytes=16 << 20),
        name="project",
    )(out_weight, *parts)
    odd_sum = odd_own + other_core(odd_send)
    rest_got = other_core(rest_send)
    twos = len(range(2, reach, 4))
    first = onward(odd_sum, 1)
    even = rest_own[:twos] + rest_got[:twos] + first[:twos]
    fours = rest_own[twos:] + rest_got[twos:] + first[twos:]
    second = onward(even, 2)
    last = fours.shape[0] - 1
    carry = fours[last] + second[last]
    for place in reversed(range(last)):
        carry = onward(carry, 4) + (fours[place] + second[place])
    half = width // n_seq
    mine = jnp.where(seq_index == 1, carry[:, half:], carry[:, :half])
    theirs = jnp.where(seq_index == 1, carry[:, :half], carry[:, half:])
    return (mine + other_core(theirs)).astype(jnp.bfloat16)


def solution(mesh):
    return jax.shard_map(
        body,
        mesh=mesh,
        in_specs=(
            P("groups", None, None),
            P(("tensor", "seq"), "groups", None),
            P(("tensor", "seq"), "groups", None),
            P("groups"),
            P(("tensor", "seq"), None),
        ),
        out_specs=P("groups", ("tensor", "seq")),
        check_vma=False,
    )
```

```python
import functools
import math

import jax
import jax.numpy as jnp
from jax import lax
from jax.experimental import pallas as pl
from jax.experimental.pallas import tpu as pltpu
from jax.sharding import PartitionSpec as P

KVH = 8
CACHE = 4096
masked_fill = -1e30
ROWS = 8
LANES = 128


def attend_kernel(
    replicas, lengths_ref, q_hbm, k_hbm, v_hbm, keep_ref, send_ref,
    q_raw, q_all, k_all, v_all, s_ref, stats_ref, q_sem, k_sem, v_sem,
):
    step = pl.program_id(0)
    tensor_index = lax.axis_index("tensor")
    seq_index = lax.axis_index("seq")
    n_seq = lax.axis_size("seq")
    span = k_hbm.shape[0]
    batch, group, head_size = q_raw.shape
    start = (tensor_index * n_seq + seq_index) * span
    kv_head = start // CACHE
    first_slot = start % CACHE
    own = tensor_index % replicas

    def cache_copy(source, target, sem, i):
        tile = pl.ds(pl.multiple_of(i * ROWS, ROWS), ROWS)
        return pltpu.make_async_copy(source.at[:, tile, :], target.at[i], sem.at[i])

    @pl.when(step == 0)
    def _():
        heads = pl.ds(pl.multiple_of(kv_head * group, group), group)
        copy = pltpu.make_async_copy(q_hbm.at[:, heads, :], q_raw, q_sem)
        copy.start()
        for i in range(batch // ROWS):
            cache_copy(k_hbm, k_all, k_sem, i).start()
            cache_copy(v_hbm, v_all, v_sem, i).start()
        copy.wait()
        q_all[...] = q_raw[...].astype(jnp.float32).reshape(batch * group, head_size)
        stats_ref[...] = jnp.zeros_like(stats_ref)

    base = pl.multiple_of(step * ROWS * group, ROWS * group)
    pieces = []
    for place in range(group):
        which, rank = place // replicas, place % replicas
        head = 2 * (own ^ rank) + (seq_index ^ which)
        pieces.append(q_all[pl.ds(base + head, ROWS, stride=group), :])
    queries = jnp.concatenate(pieces, axis=0).astype(jnp.bfloat16)

    row = lax.broadcasted_iota(jnp.int32, (ROWS, LANES), 0)
    lane = lax.broadcasted_iota(jnp.int32, (ROWS, LANES), 1)
    left = jnp.zeros((ROWS, LANES), jnp.int32)
    for r in range(ROWS):
        left = jnp.where(row == r, lengths_ref[step * ROWS + r] - first_slot, left)
    place_of = jnp.where(lane % ROWS == row, lane // ROWS, CACHE)
    slots = LANES // ROWS
    blocks = span // slots
    per_dot = 4
    scale = math.log2(math.e) / math.sqrt(head_size)
    width = per_dot * LANES

    cache_copy(k_hbm, k_all, k_sem, step).wait()
    highest = jnp.full((group * ROWS, LANES), masked_fill, jnp.float32)
    for c in range(blocks // per_dot):
        keys = k_all[step, c * per_dot * slots : (c + 1) * per_dot * slots].reshape(width, head_size)
        scores = lax.dot_general(
            queries, keys, (((1,), (1,)), ((), ())), preferred_element_type=jnp.float32
        )
        for j in range(per_dot):
            live = place_of < left - (c * per_dot + j) * slots
            live = jnp.concatenate([live] * group, axis=0)
            part = jnp.where(live, scores[:, j * LANES : (j + 1) * LANES] * scale, masked_fill)
            s_ref[c * per_dot + j] = part
            highest = jnp.maximum(highest, part)
    top = jnp.max(highest, axis=1, keepdims=True)
    cache_copy(v_hbm, v_all, v_sem, step).wait()
    total = jnp.zeros((group * ROWS, LANES), jnp.float32)
    accum = jnp.zeros((group * ROWS, head_size), jnp.float32)
    for c in range(blocks // per_dot):
        parts = []
        for j in range(per_dot):
            live = place_of < left - (c * per_dot + j) * slots
            live = jnp.concatenate([live] * group, axis=0)
            weight = jnp.where(live, jnp.exp2(s_ref[c * per_dot + j] - top), 0.0)
            total = total + weight
            parts.append(weight.astype(jnp.bfloat16))
        values = v_all[step, c * per_dot * slots : (c + 1) * per_dot * slots].reshape(width, head_size)
        accum = accum + jnp.dot(
            jnp.concatenate(parts, axis=1), values, preferred_element_type=jnp.float32
        )
    total = jnp.sum(total, axis=1, keepdims=True)
    for place in range(group):
        which, rank = place // replicas, place % replicas
        ref = (keep_ref, send_ref)[which]
        rows = slice(place * ROWS, (place + 1) * ROWS)
        ref[rank, pl.ds(pl.multiple_of(step * ROWS, ROWS), ROWS), :] = accum[rows]
        spread = jnp.where(lane == row + step * ROWS, top[rows], 0.0)
        spread = jnp.where(lane == row + step * ROWS + batch, total[rows], spread)
        stats_ref[place] += spread

    @pl.when(step == pl.num_programs(0) - 1)
    def _():
        for place in range(group):
            which, rank = place // replicas, place % replicas
            ref = (keep_ref, send_ref)[which]
            line = jnp.sum(stats_ref[place], axis=0, keepdims=True)
            ref[rank, batch:, :] = jnp.broadcast_to(line, (ROWS, LANES))


def column(line, batch):
    row = lax.broadcasted_iota(jnp.int32, (batch, LANES), 0)
    lane = lax.broadcasted_iota(jnp.int32, (batch, LANES), 1)
    return jnp.sum(jnp.where(lane == row, line, 0.0), axis=1, keepdims=True)


def merge_kernel(keep_ref, got_ref, *out_refs):
    batch = keep_ref.shape[1] - ROWS
    lane = lax.broadcasted_iota(jnp.int32, (1, LANES), 1)
    for rank, out_ref in enumerate(out_refs):
        first = keep_ref[rank, batch : batch + 1, :]
        second = got_ref[rank, batch : batch + 1, :]
        top = jnp.maximum(first, second)
        scale_a = jnp.where(lane < batch, jnp.exp2(first - top), 0.0)
        scale_b = jnp.where(lane < batch, jnp.exp2(second - top), 0.0)
        total = first * pltpu.roll(scale_a, batch, 1) + second * pltpu.roll(scale_b, batch, 1)
        out_ref[:batch, :] = keep_ref[rank, :batch, :] * column(scale_a, batch) + got_ref[
            rank, :batch, :
        ] * column(scale_b, batch)
        out_ref[batch:, :] = jnp.broadcast_to(jnp.where(lane < batch, top, total), (ROWS, LANES))


NEAR = 2
STRIDE = 2 * NEAR + 1


def plan(n_tensor):
    turns = -(-(n_tensor // 2 - NEAR) // STRIDE)
    reached = {0}
    chunks = {}
    for hop in range(NEAR + 1):
        chunks[hop] = []
        for turn in range(-turns if hop else 1, turns + 1):
            live = []
            for sign in (1, -1):
                chip = sign * (STRIDE * turn + hop) % n_tensor
                live.insert(0, chip not in reached)
                reached.add(chip)
            if any(live):
                chunks[hop].append((turn, tuple(live)))
    assert len(reached) == n_tensor
    return turns, chunks


def project_kernel(w_ref, *refs):
    n_out = 1 + 2 * (NEAR + 1)
    parts, (centre_ref, *out_refs) = refs[:-n_out], refs[-n_out:]
    tensor_index = lax.axis_index("tensor")
    seq_index = lax.axis_index("seq")
    n_tensor = lax.axis_size("tensor")
    batch = parts[0].shape[0] - ROWS
    lane = lax.broadcasted_iota(jnp.int32, (1, LANES), 1)
    lines = [ref[batch : batch + 1, :] for ref in parts]
    top = functools.reduce(jnp.maximum, lines)
    scales = [jnp.where(lane < batch, jnp.exp2(line - top), 0.0) for line in lines]
    total = sum(line * pltpu.roll(scale, batch, 1) for line, scale in zip(lines, scales))
    total = pltpu.roll(total, LANES - batch, 1)
    accum = sum(ref[:batch, :] * column(scale, batch) for ref, scale in zip(parts, scales))
    mean = accum / column(jnp.where(lane < batch, total, 0.0), batch)
    attended = mean.astype(jnp.bfloat16)
    width = centre_ref.shape[1]

    def block(chip):
        columns = pl.ds(pl.multiple_of(chip * width, width), width)
        return jnp.dot(attended, w_ref[:, columns], preferred_element_type=jnp.float32)

    centre_ref[...] = block(tensor_index)
    _, chunks = plan(n_tensor)
    for hop in reversed(range(NEAR + 1)):
        for side in (1, 0):
            core = seq_index ^ side
            ref = out_refs[2 * hop + side]
            for place, (turn, live) in enumerate(chunks[hop]):
                ahead = STRIDE * turn + hop
                shift = jnp.where(core == 1, ahead % n_tensor, -ahead % n_tensor)
                value = block(lax.rem(tensor_index + shift, n_tensor))
                if not all(live):
                    value = jnp.where((core == 1) == live[1], value, 0.0)
                ref[place] = value


def other_core(block):
    return lax.ppermute(block, "seq", [(0, 1), (1, 0)])


def across(block, mask):
    count = lax.axis_size("tensor")
    return lax.ppermute(block, "tensor", [(i, i ^ mask) for i in range(count)])


def onward(block, hops):
    count = lax.axis_size("tensor")
    route = []
    for chip in range(count):
        route.append((2 * chip + 1, 2 * ((chip + hops) % count) + 1))
        route.append((2 * chip, 2 * ((chip - hops) % count)))
    return lax.ppermute(block, ("tensor", "seq"), route)


def body(queries, keys, values, lengths, out_weight):
    n_tensor = lax.axis_size("tensor")
    n_seq = lax.axis_size("seq")
    replicas = n_tensor // KVH
    seq_index = lax.axis_index("seq")
    span, batch, head_size = keys.shape
    group = queries.shape[1] // KVH
    vmem = pl.BlockSpec(memory_space=pltpu.VMEM)
    state = jax.ShapeDtypeStruct((replicas, batch + ROWS, head_size), jnp.float32)
    piece = jax.ShapeDtypeStruct((batch + ROWS, head_size), jnp.float32)
    whole = pl.BlockSpec(state.shape, lambda i: (0, 0, 0))
    hbm = pl.BlockSpec(memory_space=pltpu.HBM)
    keep, send = pl.pallas_call(
        functools.partial(attend_kernel, replicas),
        grid=(batch // ROWS,),
        out_shape=[state, state],
        in_specs=[pl.BlockSpec(memory_space=pltpu.SMEM), hbm, hbm, hbm],
        out_specs=[whole, whole],
        scratch_shapes=[
            pltpu.VMEM((batch, group, head_size), jnp.bfloat16),
            pltpu.VMEM((batch * group, head_size), jnp.float32),
            pltpu.VMEM((batch // ROWS, span, ROWS, head_size), jnp.bfloat16),
            pltpu.VMEM((batch // ROWS, span, ROWS, head_size), jnp.bfloat16),
            pltpu.VMEM((span * ROWS // LANES, group * ROWS, LANES), jnp.float32),
            pltpu.VMEM((group, ROWS, LANES), jnp.float32),
            pltpu.SemaphoreType.DMA,
            pltpu.SemaphoreType.DMA((batch // ROWS,)),
            pltpu.SemaphoreType.DMA((batch // ROWS,)),
        ],
        compiler_params=pltpu.CompilerParams(vmem_limit_bytes=59 << 20),
        name="attend",
    )(lengths, queries, keys, values)
    got = other_core(send)
    merged = pl.pallas_call(
        merge_kernel,
        out_shape=[piece] * replicas,
        in_specs=[vmem, vmem],
        out_specs=[vmem] * replicas,
        compiler_params=pltpu.CompilerParams(vmem_limit_bytes=4 << 20),
        name="merge",
    )(keep, got)
    parts = [merged[0]] + [across(merged[mask], mask) for mask in range(1, replicas)]

    width = out_weight.shape[1] // n_tensor
    turns, chunks = plan(n_tensor)
    centre = jax.ShapeDtypeStruct((batch, width), jnp.float32)
    shapes = [jax.ShapeDtypeStruct((len(chunks[hop]), batch, width), jnp.float32) for hop in chunks]
    centre, *blocks = pl.pallas_call(
        project_kernel,
        out_shape=[centre] + [shape for shape in shapes for _ in range(2)],
        in_specs=[vmem] * (1 + replicas),
        out_specs=[vmem] * (1 + 2 * len(shapes)),
        compiler_params=pltpu.CompilerParams(vmem_limit_bytes=16 << 20),
        name="project",
    )(out_weight, *parts)
    came = {}
    for hop in (*range(1, NEAR + 1), 0):
        summed = blocks[2 * hop] + other_core(blocks[2 * hop + 1])
        if hop:
            came[hop] = onward(summed, hop)

    def near(first, last):
        out = 0.0
        for hop in came:
            out = out + came[hop][first + turns : min(last + turns, len(chunks[hop]) - 1) + 1]
        return out

    ring = summed
    back = other_core(near(-turns, -1))
    carry = ring[turns - 1] + back[0]
    for hop in came:
        if len(chunks[hop]) > 2 * turns:
            carry = carry + came[hop][2 * turns]
    for turn in reversed(range(turns)):
        own = near(turn, turn)[0] + (ring[turn - 1] + back[turns - turn] if turn else centre)
        carry = onward(carry, STRIDE) + own
    half = width // n_seq
    mine = jnp.where(seq_index == 1, carry[:, half:], carry[:, :half])
    theirs = jnp.where(seq_index == 1, carry[:, :half], carry[:, half:])
    return (mine + other_core(theirs)).astype(jnp.bfloat16)


def solution(mesh):
    return jax.shard_map(
        body,
        mesh=mesh,
        in_specs=(
            P("groups", None, None),
            P(("tensor", "seq"), "groups", None),
            P(("tensor", "seq"), "groups", None),
            P("groups"),
            P(("tensor", "seq"), None),
        ),
        out_specs=P("groups", ("tensor", "seq")),
        check_vma=False,
    )
```

```python
import functools
import math

import jax
import jax.numpy as jnp
from jax import lax
from jax.experimental import pallas as pl
from jax.experimental.pallas import tpu as pltpu
from jax.sharding import PartitionSpec as P

KVH = 8
CACHE = 4096
masked_fill = -1e30
ROWS = 8
LANES = 128


def attend_kernel(
    replicas, lengths_ref, q_hbm, k_hbm, v_hbm, keep_ref, send_ref,
    q_raw, q_all, q_tile, k_all, v_all, s_ref, top_ref, total_ref, accum_ref, q_sem, k_sem, v_sem,
):
    tensor_index = lax.axis_index("tensor")
    seq_index = lax.axis_index("seq")
    n_seq = lax.axis_size("seq")
    span = k_hbm.shape[0]
    batch, group, head_size = q_raw.shape
    start = (tensor_index * n_seq + seq_index) * span
    kv_head = start // CACHE
    first_slot = start % CACHE
    own = tensor_index % replicas
    tiles = batch // ROWS
    rows = group * ROWS
    parts = k_sem.shape[0]
    part = span // parts

    def cache_copy(source, target, sem, i):
        slots = pl.ds(i * part, part)
        return pltpu.make_async_copy(source.at[slots], target.at[slots], sem.at[i])

    heads = pl.ds(pl.multiple_of(kv_head * group, group), group)
    q_copy = pltpu.make_async_copy(q_hbm.at[:, heads, :], q_raw, q_sem)
    q_copy.start()
    for i in range(parts):
        cache_copy(k_hbm, k_all, k_sem, i).start()
    for i in range(parts):
        cache_copy(v_hbm, v_all, v_sem, i).start()
    row = lax.broadcasted_iota(jnp.int32, (ROWS, LANES), 0)
    lane = lax.broadcasted_iota(jnp.int32, (ROWS, LANES), 1)
    place_of = jnp.where(lane % ROWS == row, lane // ROWS, CACHE)
    slots = LANES // ROWS
    blocks = part // slots
    scale = math.log2(math.e) / math.sqrt(head_size)
    lefts = []
    for tile in range(tiles):
        left = jnp.zeros((ROWS, LANES), jnp.int32)
        for r in range(ROWS):
            left = jnp.where(row == r, lengths_ref[tile * ROWS + r] - first_slot, left)
        lefts.append(left)

    def live_at(tile, block):
        live = place_of < lefts[tile] - block * slots
        return jnp.concatenate([live] * group, axis=0)

    q_copy.wait()
    q_all[...] = q_raw[...].astype(jnp.float32).reshape(batch * group, head_size)
    for tile in range(tiles):
        pieces = []
        for place in range(group):
            which, rank = place // replicas, place % replicas
            head = 2 * (own ^ rank) + (seq_index ^ which)
            pieces.append(q_all[pl.ds(tile * rows + head, ROWS, stride=group), :])
        q_tile[tile] = jnp.concatenate(pieces, axis=0).astype(jnp.bfloat16)

    for i in range(parts):
        cache_copy(k_hbm, k_all, k_sem, i).wait()
        for tile in range(tiles):
            keys = k_all[i * part : (i + 1) * part, tile * ROWS : (tile + 1) * ROWS, :]
            scores = lax.dot_general(
                q_tile[tile],
                keys.reshape(part * ROWS, head_size),
                (((1,), (1,)), ((), ())),
                preferred_element_type=jnp.float32,
            )
            highest = top_ref[tile] if i else jnp.full((rows, LANES), masked_fill, jnp.float32)
            for j in range(blocks):
                score = scores[:, j * LANES : (j + 1) * LANES] * scale
                score = jnp.where(live_at(tile, i * blocks + j), score, masked_fill)
                s_ref[tile, i * blocks + j] = score
                highest = jnp.maximum(highest, score)
            top_ref[tile] = highest
    tops = [jnp.max(top_ref[tile], axis=1, keepdims=True) for tile in range(tiles)]
    for tile in range(tiles):
        top_ref[tile] = jnp.broadcast_to(tops[tile], (rows, LANES))
    for i in range(parts):
        cache_copy(v_hbm, v_all, v_sem, i).wait()
        for tile in range(tiles):
            top = top_ref[tile]
            total = total_ref[tile] if i else jnp.zeros((rows, LANES), jnp.float32)
            weights = []
            for j in range(blocks):
                weight = jnp.exp2(s_ref[tile, i * blocks + j] - top)
                weight = jnp.where(live_at(tile, i * blocks + j), weight, 0.0)
                total = total + weight
                weights.append(weight.astype(jnp.bfloat16))
            total_ref[tile] = total
            values = v_all[i * part : (i + 1) * part, tile * ROWS : (tile + 1) * ROWS, :]
            accum = jnp.dot(
                jnp.concatenate(weights, axis=1),
                values.reshape(part * ROWS, head_size),
                preferred_element_type=jnp.float32,
            )
            accum_ref[tile] = accum_ref[tile] + accum if i else accum
    lines = [jnp.zeros((ROWS, LANES), jnp.float32)] * group
    for tile in range(tiles):
        top = top_ref[tile]
        total = jnp.sum(total_ref[tile], axis=1, keepdims=True)
        for place in range(group):
            which, rank = place // replicas, place % replicas
            ref = (keep_ref, send_ref)[which]
            mine = slice(place * ROWS, (place + 1) * ROWS)
            ref[rank, tile * ROWS : (tile + 1) * ROWS, :] = accum_ref[tile, mine]
            line = jnp.where(lane == row + tile * ROWS, top[mine], lines[place])
            lines[place] = jnp.where(lane == row + tile * ROWS + batch, total[mine], line)
    for place in range(group):
        which, rank = place // replicas, place % replicas
        ref = (keep_ref, send_ref)[which]
        line = jnp.sum(lines[place], axis=0, keepdims=True)
        ref[rank, batch:, :] = jnp.broadcast_to(line, (ROWS, LANES))


def column(line, batch):
    row = lax.broadcasted_iota(jnp.int32, (batch, LANES), 0)
    lane = lax.broadcasted_iota(jnp.int32, (batch, LANES), 1)
    return jnp.sum(jnp.where(lane == row, line, 0.0), axis=1, keepdims=True)


def merge_kernel(keep_ref, got_ref, *out_refs):
    batch = keep_ref.shape[1] - ROWS
    lane = lax.broadcasted_iota(jnp.int32, (1, LANES), 1)
    for rank, out_ref in enumerate(out_refs):
        first = keep_ref[rank, batch : batch + 1, :]
        second = got_ref[rank, batch : batch + 1, :]
        top = jnp.maximum(first, second)
        scale_a = jnp.where(lane < batch, jnp.exp2(first - top), 0.0)
        scale_b = jnp.where(lane < batch, jnp.exp2(second - top), 0.0)
        total = first * pltpu.roll(scale_a, batch, 1) + second * pltpu.roll(scale_b, batch, 1)
        out_ref[:batch, :] = keep_ref[rank, :batch, :] * column(scale_a, batch) + got_ref[
            rank, :batch, :
        ] * column(scale_b, batch)
        out_ref[batch:, :] = jnp.broadcast_to(jnp.where(lane < batch, top, total), (ROWS, LANES))


NEAR = 2
STRIDE = 2 * NEAR + 1
BUNDLES = ((2, -2), (1, -1, 0))


def plan(n_tensor):
    turns = -(-(n_tensor // 2 - NEAR) // STRIDE)
    reached = {0}
    chunks = {hop: [] for bundle in BUNDLES for hop in bundle}
    for ahead in range(1, STRIDE * turns + NEAR + 1):
        turn = (ahead + NEAR) // STRIDE
        live = []
        for sign in (1, -1):
            chip = sign * ahead % n_tensor
            live.insert(0, chip not in reached)
            reached.add(chip)
        if any(live):
            chunks[ahead - STRIDE * turn].append((turn, tuple(live)))
    assert len(reached) == n_tensor
    return turns, chunks


def project_kernel(w_ref, *refs):
    n_out = 1 + 2 * len(BUNDLES)
    parts, (centre_ref, *out_refs) = refs[:-n_out], refs[-n_out:]
    tensor_index = lax.axis_index("tensor")
    seq_index = lax.axis_index("seq")
    n_tensor = lax.axis_size("tensor")
    batch = parts[0].shape[0] - ROWS
    lane = lax.broadcasted_iota(jnp.int32, (1, LANES), 1)
    lines = [ref[batch : batch + 1, :] for ref in parts]
    top = functools.reduce(jnp.maximum, lines)
    scales = [jnp.where(lane < batch, jnp.exp2(line - top), 0.0) for line in lines]
    total = sum(line * pltpu.roll(scale, batch, 1) for line, scale in zip(lines, scales))
    total = pltpu.roll(total, LANES - batch, 1)
    accum = sum(ref[:batch, :] * column(scale, batch) for ref, scale in zip(parts, scales))
    mean = accum / column(jnp.where(lane < batch, total, 0.0), batch)
    attended = mean.astype(jnp.bfloat16)
    width = centre_ref.shape[1]

    def block(chip):
        columns = pl.ds(pl.multiple_of(chip * width, width), width)
        return jnp.dot(attended, w_ref[:, columns], preferred_element_type=jnp.float32)

    centre_ref[...] = block(tensor_index)
    _, chunks = plan(n_tensor)
    for index, bundle in enumerate(BUNDLES):
        for side in (1, 0):
            core = seq_index ^ side
            ref = out_refs[2 * index + side]
            members = [(hop, *chunk) for hop in bundle for chunk in chunks[hop]]
            for place, (hop, turn, live) in enumerate(members):
                ahead = STRIDE * turn + hop
                shift = jnp.where(core == 1, ahead % n_tensor, -ahead % n_tensor)
                value = block(lax.rem(tensor_index + shift, n_tensor))
                if not all(live):
                    value = jnp.where((core == 1) == live[1], value, 0.0)
                ref[place] = value


def other_core(block):
    return lax.ppermute(block, "seq", [(0, 1), (1, 0)])


def across(block, mask):
    count = lax.axis_size("tensor")
    return lax.ppermute(block, "tensor", [(i, i ^ mask) for i in range(count)])


def onward(block, hops):
    count = lax.axis_size("tensor")
    route = []
    for chip in range(count):
        route.append((2 * chip + 1, 2 * ((chip + hops) % count) + 1))
        route.append((2 * chip, 2 * ((chip - hops) % count)))
    return lax.ppermute(block, ("tensor", "seq"), route)


def body(queries, keys, values, lengths, out_weight):
    n_tensor = lax.axis_size("tensor")
    n_seq = lax.axis_size("seq")
    replicas = n_tensor // KVH
    seq_index = lax.axis_index("seq")
    span, batch, head_size = keys.shape
    group = queries.shape[1] // KVH
    vmem = pl.BlockSpec(memory_space=pltpu.VMEM)
    state = jax.ShapeDtypeStruct((replicas, batch + ROWS, head_size), jnp.float32)
    piece = jax.ShapeDtypeStruct((batch + ROWS, head_size), jnp.float32)
    hbm = pl.BlockSpec(memory_space=pltpu.HBM)
    tiles, rows, pieces = batch // ROWS, group * ROWS, 4
    keep, send = pl.pallas_call(
        functools.partial(attend_kernel, replicas),
        out_shape=[state, state],
        in_specs=[pl.BlockSpec(memory_space=pltpu.SMEM), hbm, hbm, hbm],
        out_specs=[vmem, vmem],
        scratch_shapes=[
            pltpu.VMEM((batch, group, head_size), jnp.bfloat16),
            pltpu.VMEM((batch * group, head_size), jnp.float32),
            pltpu.VMEM((tiles, rows, head_size), jnp.bfloat16),
            pltpu.VMEM(keys.shape, jnp.bfloat16),
            pltpu.VMEM(values.shape, jnp.bfloat16),
            pltpu.VMEM((tiles, span * ROWS // LANES, rows, LANES), jnp.float32),
            pltpu.VMEM((tiles, rows, LANES), jnp.float32),
            pltpu.VMEM((tiles, rows, LANES), jnp.float32),
            pltpu.VMEM((tiles, rows, head_size), jnp.float32),
            pltpu.SemaphoreType.DMA,
            pltpu.SemaphoreType.DMA((pieces,)),
            pltpu.SemaphoreType.DMA((pieces,)),
        ],
        compiler_params=pltpu.CompilerParams(vmem_limit_bytes=59 << 20),
        name="attend",
    )(lengths, queries, keys, values)
    got = other_core(send)
    merged = pl.pallas_call(
        merge_kernel,
        out_shape=[piece] * replicas,
        in_specs=[vmem, vmem],
        out_specs=[vmem] * replicas,
        compiler_params=pltpu.CompilerParams(vmem_limit_bytes=4 << 20),
        name="merge",
    )(keep, got)
    parts = [merged[0]] + [across(merged[mask], mask) for mask in reversed(range(1, replicas))]

    width = out_weight.shape[1] // n_tensor
    turns, chunks = plan(n_tensor)
    centre = jax.ShapeDtypeStruct((batch, width), jnp.float32)
    counts = [sum(len(chunks[hop]) for hop in bundle) for bundle in BUNDLES]
    shapes = [jax.ShapeDtypeStruct((count, batch, width), jnp.float32) for count in counts]
    centre, *blocks = pl.pallas_call(
        project_kernel,
        out_shape=[centre] + [shape for shape in shapes for _ in range(2)],
        in_specs=[vmem] * (1 + replicas),
        out_specs=[vmem] * (1 + 2 * len(shapes)),
        compiler_params=pltpu.CompilerParams(vmem_limit_bytes=16 << 20),
        name="project",
    )(out_weight, *parts)
    came = {}
    swapped = [other_core(block) for block in blocks[1::2]]
    for bundle, mine, theirs in zip(BUNDLES, blocks[::2], swapped):
        first = 0
        for hop in bundle:
            last = first + len(chunks[hop])
            summed = mine[first:last] + theirs[first:last]
            came[hop] = onward(summed, hop) if hop else summed
            first = last

    def near(turn):
        out = 0.0 if turn else centre
        for hop in came:
            for place, (at, _) in enumerate(chunks[hop]):
                if at == turn:
                    out = out + came[hop][place]
        return out

    carry = near(turns)
    for turn in reversed(range(turns)):
        carry = onward(carry, STRIDE) + near(turn)
    half = width // n_seq
    mine = jnp.where(seq_index == 1, carry[:, half:], carry[:, :half])
    theirs = jnp.where(seq_index == 1, carry[:, :half], carry[:, half:])
    return (mine + other_core(theirs)).astype(jnp.bfloat16)


def solution(mesh):
    return jax.shard_map(
        body,
        mesh=mesh,
        in_specs=(
            P("groups", None, None),
            P(("tensor", "seq"), "groups", None),
            P(("tensor", "seq"), "groups", None),
            P("groups"),
            P(("tensor", "seq"), None),
        ),
        out_specs=P("groups", ("tensor", "seq")),
        check_vma=False,
    )
```

```python
import functools
import math

import jax
import jax.numpy as jnp
from jax import lax
from jax.experimental import pallas as pl
from jax.experimental.pallas import tpu as pltpu
from jax.sharding import PartitionSpec as P

KVH = 8
CACHE = 4096
masked_fill = -1e30
ROWS = 8
LANES = 128
PIECES = 4
AHEAD = 3


def attend_kernel(
    replicas, lengths_hbm, q_hbm, k_hbm, v_hbm, keep_ref, send_ref,
    q_raw, q_all, q_tile, k_all, v_all, s_ref, top_ref, total_ref, accum_ref, lengths_ref, q_sem, k_sem, v_sem, l_sem,
):
    tensor_index = lax.axis_index("tensor")
    seq_index = lax.axis_index("seq")
    n_seq = lax.axis_size("seq")
    span = k_hbm.shape[0]
    batch, group, head_size = q_raw.shape
    start = (tensor_index * n_seq + seq_index) * span
    kv_head = start // CACHE
    first_slot = start % CACHE
    own = tensor_index % replicas
    tiles = batch // ROWS
    rows = group * ROWS
    parts = k_sem.shape[0]
    part = span // parts

    def cache_copy(source, target, sem, i):
        slots = pl.ds(i * part, part)
        return pltpu.make_async_copy(source.at[slots], target.at[slots], sem.at[i])

    heads = pl.ds(pl.multiple_of(kv_head * group, group), group)
    q_copy = pltpu.make_async_copy(q_hbm.at[:, heads, :], q_raw, q_sem)
    q_copy.start()
    l_copy = pltpu.make_async_copy(lengths_hbm, lengths_ref, l_sem)
    l_copy.start()
    copies = [cache_copy(k_hbm, k_all, k_sem, i) for i in range(parts)]
    copies += [cache_copy(v_hbm, v_all, v_sem, i) for i in range(parts)]
    for copy in copies[:AHEAD]:
        copy.start()

    def arrived(index):
        copies[index].wait()
        if index + AHEAD < len(copies):
            copies[index + AHEAD].start()

    row = lax.broadcasted_iota(jnp.int32, (ROWS, LANES), 0)
    lane = lax.broadcasted_iota(jnp.int32, (ROWS, LANES), 1)
    place_of = jnp.where(lane % ROWS == row, lane // ROWS, CACHE)
    slots = LANES // ROWS
    blocks = part // slots
    scale = math.log2(math.e) / math.sqrt(head_size)
    l_copy.wait()
    lefts = []
    for tile in range(tiles):
        left = jnp.zeros((ROWS, LANES), jnp.int32)
        for r in range(ROWS):
            left = jnp.where(row == r, lengths_ref[tile * ROWS + r] - first_slot, left)
        lefts.append(left)

    def live_at(tile, block):
        live = place_of < lefts[tile] - block * slots
        return jnp.concatenate([live] * group, axis=0)

    q_copy.wait()
    q_all[...] = q_raw[...].astype(jnp.float32).reshape(batch * group, head_size)
    for tile in range(tiles):
        pieces = []
        for place in range(group):
            which, rank = place // replicas, place % replicas
            head = 2 * (own ^ rank) + (seq_index ^ which)
            pieces.append(q_all[pl.ds(tile * rows + head, ROWS, stride=group), :])
        q_tile[tile] = jnp.concatenate(pieces, axis=0).astype(jnp.bfloat16)

    for i in range(parts):
        arrived(i)
        for tile in range(tiles):
            keys = k_all[i * part : (i + 1) * part, tile * ROWS : (tile + 1) * ROWS, :]
            scores = lax.dot_general(
                q_tile[tile],
                keys.reshape(part * ROWS, head_size),
                (((1,), (1,)), ((), ())),
                preferred_element_type=jnp.float32,
            )
            highest = top_ref[tile] if i else jnp.full((rows, LANES), masked_fill, jnp.float32)
            for j in range(blocks):
                score = scores[:, j * LANES : (j + 1) * LANES] * scale
                score = jnp.where(live_at(tile, i * blocks + j), score, masked_fill)
                s_ref[tile, i * blocks + j] = score
                highest = jnp.maximum(highest, score)
            top_ref[tile] = highest
    tops = [jnp.max(top_ref[tile], axis=1, keepdims=True) for tile in range(tiles)]
    for tile in range(tiles):
        top_ref[tile] = jnp.broadcast_to(tops[tile], (rows, LANES))
    for i in range(parts):
        arrived(parts + i)
        for tile in range(tiles):
            top = top_ref[tile]
            total = total_ref[tile] if i else jnp.zeros((rows, LANES), jnp.float32)
            weights = []
            for j in range(blocks):
                weight = jnp.exp2(s_ref[tile, i * blocks + j] - top)
                weight = jnp.where(live_at(tile, i * blocks + j), weight, 0.0)
                total = total + weight
                weights.append(weight.astype(jnp.bfloat16))
            total_ref[tile] = total
            values = v_all[i * part : (i + 1) * part, tile * ROWS : (tile + 1) * ROWS, :]
            accum = jnp.dot(
                jnp.concatenate(weights, axis=1),
                values.reshape(part * ROWS, head_size),
                preferred_element_type=jnp.float32,
            )
            accum_ref[tile] = accum_ref[tile] + accum if i else accum
    lines = [jnp.zeros((ROWS, LANES), jnp.float32)] * group
    for tile in range(tiles):
        top = top_ref[tile]
        total = jnp.sum(total_ref[tile], axis=1, keepdims=True)
        for place in range(group):
            which, rank = place // replicas, place % replicas
            ref = (keep_ref, send_ref)[which]
            mine = slice(place * ROWS, (place + 1) * ROWS)
            ref[rank, tile * ROWS : (tile + 1) * ROWS, :] = accum_ref[tile, mine]
            line = jnp.where(lane == row + tile * ROWS, top[mine], lines[place])
            lines[place] = jnp.where(lane == row + tile * ROWS + batch, total[mine], line)
    for place in range(group):
        which, rank = place // replicas, place % replicas
        ref = (keep_ref, send_ref)[which]
        line = jnp.sum(lines[place], axis=0, keepdims=True)
        ref[rank, batch:, :] = jnp.broadcast_to(line, (ROWS, LANES))


def column(line, batch):
    row = lax.broadcasted_iota(jnp.int32, (batch, LANES), 0)
    lane = lax.broadcasted_iota(jnp.int32, (batch, LANES), 1)
    return jnp.sum(jnp.where(lane == row, line, 0.0), axis=1, keepdims=True)


def merge_kernel(keep_ref, got_ref, *out_refs):
    batch = keep_ref.shape[1] - ROWS
    lane = lax.broadcasted_iota(jnp.int32, (1, LANES), 1)
    for rank, out_ref in enumerate(out_refs):
        first = keep_ref[rank, batch : batch + 1, :]
        second = got_ref[rank, batch : batch + 1, :]
        top = jnp.maximum(first, second)
        scale_a = jnp.where(lane < batch, jnp.exp2(first - top), 0.0)
        scale_b = jnp.where(lane < batch, jnp.exp2(second - top), 0.0)
        total = first * pltpu.roll(scale_a, batch, 1) + second * pltpu.roll(scale_b, batch, 1)
        out_ref[:batch, :] = keep_ref[rank, :batch, :] * column(scale_a, batch) + got_ref[
            rank, :batch, :
        ] * column(scale_b, batch)
        out_ref[batch:, :] = jnp.broadcast_to(jnp.where(lane < batch, top, total), (ROWS, LANES))


NEAR = 2
STRIDE = 2 * NEAR + 1
BUNDLES = ((2, -2), (1, -1, 0))


def plan(n_tensor):
    turns = -(-(n_tensor // 2 - NEAR) // STRIDE)
    reached = {0}
    chunks = {hop: [] for bundle in BUNDLES for hop in bundle}
    for ahead in range(1, STRIDE * turns + NEAR + 1):
        turn = (ahead + NEAR) // STRIDE
        live = []
        for sign in (1, -1):
            chip = sign * ahead % n_tensor
            live.insert(0, chip not in reached)
            reached.add(chip)
        if any(live):
            chunks[ahead - STRIDE * turn].append((turn, tuple(live)))
    assert len(reached) == n_tensor
    return turns, chunks


def project_kernel(w_ref, *refs):
    n_out = 1 + 2 * len(BUNDLES)
    parts, (centre_ref, *out_refs) = refs[:-n_out], refs[-n_out:]
    tensor_index = lax.axis_index("tensor")
    seq_index = lax.axis_index("seq")
    n_tensor = lax.axis_size("tensor")
    batch = parts[0].shape[0] - ROWS
    lane = lax.broadcasted_iota(jnp.int32, (1, LANES), 1)
    lines = [ref[batch : batch + 1, :] for ref in parts]
    top = functools.reduce(jnp.maximum, lines)
    scales = [jnp.where(lane < batch, jnp.exp2(line - top), 0.0) for line in lines]
    total = sum(line * pltpu.roll(scale, batch, 1) for line, scale in zip(lines, scales))
    total = pltpu.roll(total, LANES - batch, 1)
    accum = sum(ref[:batch, :] * column(scale, batch) for ref, scale in zip(parts, scales))
    mean = accum / column(jnp.where(lane < batch, total, 0.0), batch)
    attended = mean.astype(jnp.bfloat16)
    width = centre_ref.shape[1]

    def block(chip):
        columns = pl.ds(pl.multiple_of(chip * width, width), width)
        return jnp.dot(attended, w_ref[:, columns], preferred_element_type=jnp.float32)

    centre_ref[...] = block(tensor_index)
    _, chunks = plan(n_tensor)
    for index, bundle in enumerate(BUNDLES):
        for side in (1, 0):
            core = seq_index ^ side
            ref = out_refs[2 * index + side]
            members = [(hop, *chunk) for hop in bundle for chunk in chunks[hop]]
            for place, (hop, turn, live) in enumerate(members):
                ahead = STRIDE * turn + hop
                shift = jnp.where(core == 1, ahead % n_tensor, -ahead % n_tensor)
                value = block(lax.rem(tensor_index + shift, n_tensor))
                if not all(live):
                    value = jnp.where((core == 1) == live[1], value, 0.0)
                ref[place] = value


def other_core(block):
    return lax.ppermute(block, "seq", [(0, 1), (1, 0)])


def across(block, mask):
    count = lax.axis_size("tensor")
    return lax.ppermute(block, "tensor", [(i, i ^ mask) for i in range(count)])


def onward(block, hops):
    count = lax.axis_size("tensor")
    route = []
    for chip in range(count):
        route.append((2 * chip + 1, 2 * ((chip + hops) % count) + 1))
        route.append((2 * chip, 2 * ((chip - hops) % count)))
    return lax.ppermute(block, ("tensor", "seq"), route)


def body(queries, keys, values, lengths, out_weight):
    n_tensor = lax.axis_size("tensor")
    n_seq = lax.axis_size("seq")
    replicas = n_tensor // KVH
    seq_index = lax.axis_index("seq")
    span, batch, head_size = keys.shape
    group = queries.shape[1] // KVH
    vmem = pl.BlockSpec(memory_space=pltpu.VMEM)
    state = jax.ShapeDtypeStruct((replicas, batch + ROWS, head_size), jnp.float32)
    piece = jax.ShapeDtypeStruct((batch + ROWS, head_size), jnp.float32)
    hbm = pl.BlockSpec(memory_space=pltpu.HBM)
    tiles, rows = batch // ROWS, group * ROWS
    keep, send = pl.pallas_call(
        functools.partial(attend_kernel, replicas),
        out_shape=[state, state],
        in_specs=[hbm] * 4,
        out_specs=[vmem, vmem],
        scratch_shapes=[
            pltpu.VMEM((batch, group, head_size), jnp.bfloat16),
            pltpu.VMEM((batch * group, head_size), jnp.float32),
            pltpu.VMEM((tiles, rows, head_size), jnp.bfloat16),
            pltpu.VMEM(keys.shape, jnp.bfloat16),
            pltpu.VMEM(values.shape, jnp.bfloat16),
            pltpu.VMEM((tiles, span * ROWS // LANES, rows, LANES), jnp.float32),
            pltpu.VMEM((tiles, rows, LANES), jnp.float32),
            pltpu.VMEM((tiles, rows, LANES), jnp.float32),
            pltpu.VMEM((tiles, rows, head_size), jnp.float32),
            pltpu.SMEM((batch,), jnp.int32),
            pltpu.SemaphoreType.DMA,
            pltpu.SemaphoreType.DMA((PIECES,)),
            pltpu.SemaphoreType.DMA((PIECES,)),
            pltpu.SemaphoreType.DMA,
        ],
        compiler_params=pltpu.CompilerParams(vmem_limit_bytes=24 << 20),
        name="attend",
    )(*[pltpu.with_memory_space_constraint(x, pltpu.HBM) for x in (lengths, queries, keys, values)])
    got = other_core(send)
    merged = pl.pallas_call(
        merge_kernel,
        out_shape=[piece] * replicas,
        in_specs=[vmem, vmem],
        out_specs=[vmem] * replicas,
        compiler_params=pltpu.CompilerParams(vmem_limit_bytes=4 << 20),
        name="merge",
    )(keep, got)
    parts = [merged[0]] + [across(merged[mask], mask) for mask in reversed(range(1, replicas))]

    width = out_weight.shape[1] // n_tensor
    turns, chunks = plan(n_tensor)
    centre = jax.ShapeDtypeStruct((batch, width), jnp.float32)
    counts = [sum(len(chunks[hop]) for hop in bundle) for bundle in BUNDLES]
    shapes = [jax.ShapeDtypeStruct((count, batch, width), jnp.float32) for count in counts]
    centre, *blocks = pl.pallas_call(
        project_kernel,
        out_shape=[centre] + [shape for shape in shapes for _ in range(2)],
        in_specs=[vmem] * (1 + replicas),
        out_specs=[vmem] * (1 + 2 * len(shapes)),
        compiler_params=pltpu.CompilerParams(vmem_limit_bytes=16 << 20),
        name="project",
    )(out_weight, *parts)
    came = {}
    swapped = [other_core(block) for block in blocks[1::2]]
    for bundle, mine, theirs in zip(BUNDLES, blocks[::2], swapped):
        first = 0
        for hop in bundle:
            last = first + len(chunks[hop])
            summed = mine[first:last] + theirs[first:last]
            came[hop] = onward(summed, hop) if hop else summed
            first = last

    def near(turn):
        out = 0.0 if turn else centre
        for hop in came:
            for place, (at, _) in enumerate(chunks[hop]):
                if at == turn:
                    out = out + came[hop][place]
        return out

    carry = near(turns)
    for turn in reversed(range(turns)):
        carry = onward(carry, STRIDE) + near(turn)
    half = width // n_seq
    mine = jnp.where(seq_index == 1, carry[:, half:], carry[:, :half])
    theirs = jnp.where(seq_index == 1, carry[:, :half], carry[:, half:])
    return (mine + other_core(theirs)).astype(jnp.bfloat16)


def solution(mesh):
    return jax.shard_map(
        body,
        mesh=mesh,
        in_specs=(
            P("groups", None, None),
            P(("tensor", "seq"), "groups", None),
            P(("tensor", "seq"), "groups", None),
            P("groups"),
            P(("tensor", "seq"), None),
        ),
        out_specs=P("groups", ("tensor", "seq")),
        check_vma=False,
    )
```

```python
import functools
import math

import jax
import jax.numpy as jnp
from jax import lax
from jax.experimental import pallas as pl
from jax.experimental.pallas import tpu as pltpu
from jax.sharding import PartitionSpec as P

KVH = 8
CACHE = 4096
masked_fill = -1e30
ROWS = 8
LANES = 128
PIECES = 4
AHEAD = 3


def attend_kernel(
    replicas, lengths_hbm, q_hbm, k_hbm, v_hbm, keep_ref, send_ref,
    q_raw, q_all, q_tile, k_all, v_all, s_ref, top_ref, total_ref, accum_ref, lengths_ref, q_sem, k_sem, v_sem, l_sem,
):
    tensor_index = lax.axis_index("tensor")
    seq_index = lax.axis_index("seq")
    n_seq = lax.axis_size("seq")
    span = k_hbm.shape[0]
    batch, group, head_size = q_raw.shape
    start = (tensor_index * n_seq + seq_index) * span
    kv_head = start // CACHE
    first_slot = start % CACHE
    own = tensor_index % replicas
    tiles = batch // ROWS
    rows = group * ROWS
    parts = k_sem.shape[0]
    part = span // parts

    def cache_copy(source, target, sem, i):
        slots = pl.ds(i * part, part)
        return pltpu.make_async_copy(source.at[slots], target.at[slots], sem.at[i])

    heads = pl.ds(pl.multiple_of(kv_head * group, group), group)
    q_copy = pltpu.make_async_copy(q_hbm.at[:, heads, :], q_raw, q_sem)
    q_copy.start()
    l_copy = pltpu.make_async_copy(lengths_hbm, lengths_ref, l_sem)
    l_copy.start()
    copies = [cache_copy(k_hbm, k_all, k_sem, i) for i in range(parts)]
    copies += [cache_copy(v_hbm, v_all, v_sem, i) for i in range(parts)]
    for copy in copies[:AHEAD]:
        copy.start()

    def arrived(index):
        copies[index].wait()
        if index + AHEAD < len(copies):
            copies[index + AHEAD].start()

    row = lax.broadcasted_iota(jnp.int32, (ROWS, LANES), 0)
    lane = lax.broadcasted_iota(jnp.int32, (ROWS, LANES), 1)
    place_of = jnp.where(lane % ROWS == row, lane // ROWS, CACHE)
    slots = LANES // ROWS
    blocks = part // slots
    scale = math.log2(math.e) / math.sqrt(head_size)
    l_copy.wait()
    lefts = []
    for tile in range(tiles):
        left = jnp.zeros((ROWS, LANES), jnp.int32)
        for r in range(ROWS):
            left = jnp.where(row == r, lengths_ref[tile * ROWS + r] - first_slot, left)
        lefts.append(left)

    def live_at(tile, block):
        live = place_of < lefts[tile] - block * slots
        return jnp.concatenate([live] * group, axis=0)

    q_copy.wait()
    q_all[...] = q_raw[...].astype(jnp.float32).reshape(batch * group, head_size)
    for tile in range(tiles):
        pieces = []
        for place in range(group):
            which, rank = place // replicas, place % replicas
            head = 2 * (own ^ rank) + (seq_index ^ which)
            pieces.append(q_all[pl.ds(tile * rows + head, ROWS, stride=group), :])
        q_tile[tile] = jnp.concatenate(pieces, axis=0).astype(jnp.bfloat16)

    for i in range(parts):
        arrived(i)
        for tile in range(tiles):
            keys = k_all[i * part : (i + 1) * part, tile * ROWS : (tile + 1) * ROWS, :]
            scores = lax.dot_general(
                q_tile[tile],
                keys.reshape(part * ROWS, head_size),
                (((1,), (1,)), ((), ())),
                preferred_element_type=jnp.float32,
            )
            highest = top_ref[tile] if i else jnp.full((rows, LANES), masked_fill, jnp.float32)
            for j in range(blocks):
                score = scores[:, j * LANES : (j + 1) * LANES] * scale
                score = jnp.where(live_at(tile, i * blocks + j), score, masked_fill)
                s_ref[tile, i * blocks + j] = score
                highest = jnp.maximum(highest, score)
            top_ref[tile] = highest
    tops = [jnp.max(top_ref[tile], axis=1, keepdims=True) for tile in range(tiles)]
    for tile in range(tiles):
        top_ref[tile] = jnp.broadcast_to(tops[tile], (rows, LANES))
    for i in range(parts):
        arrived(parts + i)
        for tile in range(tiles):
            top = top_ref[tile]
            total = total_ref[tile] if i else jnp.zeros((rows, LANES), jnp.float32)
            weights = []
            for j in range(blocks):
                weight = jnp.exp2(s_ref[tile, i * blocks + j] - top)
                weight = jnp.where(live_at(tile, i * blocks + j), weight, 0.0)
                total = total + weight
                weights.append(weight.astype(jnp.bfloat16))
            total_ref[tile] = total
            values = v_all[i * part : (i + 1) * part, tile * ROWS : (tile + 1) * ROWS, :]
            accum = jnp.dot(
                jnp.concatenate(weights, axis=1),
                values.reshape(part * ROWS, head_size),
                preferred_element_type=jnp.float32,
            )
            accum_ref[tile] = accum_ref[tile] + accum if i else accum
    lines = [jnp.zeros((ROWS, LANES), jnp.float32)] * group
    for tile in range(tiles):
        top = top_ref[tile]
        total = jnp.sum(total_ref[tile], axis=1, keepdims=True)
        for place in range(group):
            which, rank = place // replicas, place % replicas
            ref = (keep_ref, send_ref)[which]
            mine = slice(place * ROWS, (place + 1) * ROWS)
            ref[rank, tile * ROWS : (tile + 1) * ROWS, :] = accum_ref[tile, mine]
            line = jnp.where(lane == row + tile * ROWS, top[mine], lines[place])
            lines[place] = jnp.where(lane == row + tile * ROWS + batch, total[mine], line)
    for place in range(group):
        which, rank = place // replicas, place % replicas
        ref = (keep_ref, send_ref)[which]
        line = jnp.sum(lines[place], axis=0, keepdims=True)
        ref[rank, batch:, :] = jnp.broadcast_to(line, (ROWS, LANES))


def column(line, batch):
    row = lax.broadcasted_iota(jnp.int32, (batch, LANES), 0)
    lane = lax.broadcasted_iota(jnp.int32, (batch, LANES), 1)
    return jnp.sum(jnp.where(lane == row, line, 0.0), axis=1, keepdims=True)


def merge_kernel(keep_ref, got_ref, *out_refs):
    batch = keep_ref.shape[1] - ROWS
    lane = lax.broadcasted_iota(jnp.int32, (1, LANES), 1)
    for rank, out_ref in enumerate(out_refs):
        first = keep_ref[rank, batch : batch + 1, :]
        second = got_ref[rank, batch : batch + 1, :]
        top = jnp.maximum(first, second)
        scale_a = jnp.where(lane < batch, jnp.exp2(first - top), 0.0)
        scale_b = jnp.where(lane < batch, jnp.exp2(second - top), 0.0)
        total = first * pltpu.roll(scale_a, batch, 1) + second * pltpu.roll(scale_b, batch, 1)
        out_ref[:batch, :] = keep_ref[rank, :batch, :] * column(scale_a, batch) + got_ref[
            rank, :batch, :
        ] * column(scale_b, batch)
        out_ref[batch:, :] = jnp.broadcast_to(jnp.where(lane < batch, top, total), (ROWS, LANES))


NEAR = 2
STRIDE = 2 * NEAR + 1
BUNDLES = ((-2, 1), (-1, 0, 2))


def plan(n_tensor):
    turns = -(-(n_tensor // 2 - NEAR) // STRIDE)
    reached = {0}
    chunks = {hop: [] for bundle in BUNDLES for hop in bundle}
    for ahead in range(1, STRIDE * turns + NEAR + 1):
        turn = (ahead + NEAR) // STRIDE
        live = []
        for sign in (1, -1):
            chip = sign * ahead % n_tensor
            live.insert(0, chip not in reached)
            reached.add(chip)
        if any(live):
            chunks[ahead - STRIDE * turn].append((turn, tuple(live)))
    assert len(reached) == n_tensor
    return turns, chunks


def project_kernel(w_ref, *refs):
    n_out = 1 + 2 * len(BUNDLES)
    parts, (centre_ref, *out_refs) = refs[:-n_out], refs[-n_out:]
    tensor_index = lax.axis_index("tensor")
    seq_index = lax.axis_index("seq")
    n_tensor = lax.axis_size("tensor")
    batch = parts[0].shape[0] - ROWS
    lane = lax.broadcasted_iota(jnp.int32, (1, LANES), 1)
    lines = [ref[batch : batch + 1, :] for ref in parts]
    top = functools.reduce(jnp.maximum, lines)
    scales = [jnp.where(lane < batch, jnp.exp2(line - top), 0.0) for line in lines]
    total = sum(line * pltpu.roll(scale, batch, 1) for line, scale in zip(lines, scales))
    total = pltpu.roll(total, LANES - batch, 1)
    accum = sum(ref[:batch, :] * column(scale, batch) for ref, scale in zip(parts, scales))
    mean = accum / column(jnp.where(lane < batch, total, 0.0), batch)
    attended = mean.astype(jnp.bfloat16)
    width = centre_ref.shape[1]

    def block(chip):
        columns = pl.ds(pl.multiple_of(chip * width, width), width)
        return jnp.dot(attended, w_ref[:, columns], preferred_element_type=jnp.float32)

    centre_ref[...] = block(tensor_index)
    _, chunks = plan(n_tensor)
    for index, bundle in enumerate(BUNDLES):
        for side in (1, 0):
            core = seq_index ^ side
            ref = out_refs[2 * index + side]
            members = [(hop, *chunk) for hop in bundle for chunk in chunks[hop]]
            for place, (hop, turn, live) in enumerate(members):
                ahead = STRIDE * turn + hop
                shift = jnp.where(core == 1, ahead % n_tensor, -ahead % n_tensor)
                value = block(lax.rem(tensor_index + shift, n_tensor))
                if not all(live):
                    value = jnp.where((core == 1) == live[1], value, 0.0)
                ref[place] = value


def other_core(block):
    return lax.ppermute(block, "seq", [(0, 1), (1, 0)])


def across(block, mask):
    count = lax.axis_size("tensor")
    return lax.ppermute(block, "tensor", [(i, i ^ mask) for i in range(count)])


def onward(block, hops):
    count = lax.axis_size("tensor")
    route = []
    for chip in range(count):
        route.append((2 * chip + 1, 2 * ((chip + hops) % count) + 1))
        route.append((2 * chip, 2 * ((chip - hops) % count)))
    return lax.ppermute(block, ("tensor", "seq"), route)


def body(queries, keys, values, lengths, out_weight):
    n_tensor = lax.axis_size("tensor")
    n_seq = lax.axis_size("seq")
    replicas = n_tensor // KVH
    seq_index = lax.axis_index("seq")
    span, batch, head_size = keys.shape
    group = queries.shape[1] // KVH
    vmem = pl.BlockSpec(memory_space=pltpu.VMEM)
    state = jax.ShapeDtypeStruct((replicas, batch + ROWS, head_size), jnp.float32)
    piece = jax.ShapeDtypeStruct((batch + ROWS, head_size), jnp.float32)
    hbm = pl.BlockSpec(memory_space=pltpu.HBM)
    tiles, rows = batch // ROWS, group * ROWS
    keep, send = pl.pallas_call(
        functools.partial(attend_kernel, replicas),
        out_shape=[state, state],
        in_specs=[hbm] * 4,
        out_specs=[vmem, vmem],
        scratch_shapes=[
            pltpu.VMEM((batch, group, head_size), jnp.bfloat16),
            pltpu.VMEM((batch * group, head_size), jnp.float32),
            pltpu.VMEM((tiles, rows, head_size), jnp.bfloat16),
            pltpu.VMEM(keys.shape, jnp.bfloat16),
            pltpu.VMEM(values.shape, jnp.bfloat16),
            pltpu.VMEM((tiles, span * ROWS // LANES, rows, LANES), jnp.float32),
            pltpu.VMEM((tiles, rows, LANES), jnp.float32),
            pltpu.VMEM((tiles, rows, LANES), jnp.float32),
            pltpu.VMEM((tiles, rows, head_size), jnp.float32),
            pltpu.SMEM((batch,), jnp.int32),
            pltpu.SemaphoreType.DMA,
            pltpu.SemaphoreType.DMA((PIECES,)),
            pltpu.SemaphoreType.DMA((PIECES,)),
            pltpu.SemaphoreType.DMA,
        ],
        compiler_params=pltpu.CompilerParams(vmem_limit_bytes=24 << 20),
        name="attend",
    )(*[pltpu.with_memory_space_constraint(x, pltpu.HBM) for x in (lengths, queries, keys, values)])
    got = other_core(send)
    merged = pl.pallas_call(
        merge_kernel,
        out_shape=[piece] * replicas,
        in_specs=[vmem, vmem],
        out_specs=[vmem] * replicas,
        compiler_params=pltpu.CompilerParams(vmem_limit_bytes=4 << 20),
        name="merge",
    )(keep, got)
    parts = [merged[0]] + [across(merged[mask], mask) for mask in reversed(range(1, replicas))]

    width = out_weight.shape[1] // n_tensor
    turns, chunks = plan(n_tensor)
    centre = jax.ShapeDtypeStruct((batch, width), jnp.float32)
    counts = [sum(len(chunks[hop]) for hop in bundle) for bundle in BUNDLES]
    shapes = [jax.ShapeDtypeStruct((count, batch, width), jnp.float32) for count in counts]
    centre, *blocks = pl.pallas_call(
        project_kernel,
        out_shape=[centre] + [shape for shape in shapes for _ in range(2)],
        in_specs=[vmem] * (1 + replicas),
        out_specs=[vmem] * (1 + 2 * len(shapes)),
        compiler_params=pltpu.CompilerParams(vmem_limit_bytes=16 << 20),
        name="project",
    )(out_weight, *parts)
    came = {}
    swapped = [other_core(block) for block in blocks[1::2]]
    for bundle, mine, theirs in zip(BUNDLES, blocks[::2], swapped):
        first = 0
        for hop in bundle:
            last = first + len(chunks[hop])
            summed = mine[first:last] + theirs[first:last]
            came[hop] = onward(summed, hop) if hop else summed
            first = last

    def near(turn):
        out = 0.0 if turn else centre
        for hop in came:
            for place, (at, _) in enumerate(chunks[hop]):
                if at == turn:
                    out = out + came[hop][place]
        return out

    carry = near(turns)
    for turn in reversed(range(turns)):
        carry = onward(carry, STRIDE) + near(turn)
    half = width // n_seq
    mine = jnp.where(seq_index == 1, carry[:, half:], carry[:, :half])
    theirs = jnp.where(seq_index == 1, carry[:, :half], carry[:, half:])
    return (mine + other_core(theirs)).astype(jnp.bfloat16)


def solution(mesh):
    return jax.shard_map(
        body,
        mesh=mesh,
        in_specs=(
            P("groups", None, None),
            P(("tensor", "seq"), "groups", None),
            P(("tensor", "seq"), "groups", None),
            P("groups"),
            P(("tensor", "seq"), None),
        ),
        out_specs=P("groups", ("tensor", "seq")),
        check_vma=False,
    )
```
